32 devices in a mesh: hap: 16 (over z, x, core), mk: 2 (over y).
Axes of the slice: x: 2, y: 2, z: 4, core: 2. Of those that a mesh axis runs over, the one named last changes fastest.
Arguments:
- posterior: bfloat16 [10, 1024, 16384], P('mk', None, 'hap'), may hold values from 0 to 1, as said below
- alleles: int32 [16384, 64], P('hap', 'mk'), may hold values from 0 to 1
- owner_map: int32 [1024], replicated, may hold values from 0 to 31, as said below
Outputs:
- dosage: float32 [1024, 64], P(('hap', 'mk'))
The draws below stay inside these ranges and needn't reach their ends.
Inputs may be any that keep to these rules, and one draw needn't show every extreme that they name: `owner_map`: every device index is named by exactly 32 targets. `posterior`: every entry is positive.
All inputs are finite; a program needn't handle non-finite values.
Results may differ from the reference program's by a relative error of at most 0.0003.
Values sent between devices are 32-bit elements; how exact they have to be, the bound alone decides.
A program may use at most 64 MiB of HBM per device.

```python
import jax
import jax.numpy as jnp
from jax import lax

TGT = 1024
ANCH = 5
MB = 32
MARKERS = 64
REF = 16384
TOWN = 32
N_HAP = 16
N_MK = 2


def draw_owner_map(key, part):
    return (jax.random.permutation(key, TGT) // TOWN).astype(jnp.int32)


def draw_alleles(key, part):
    level_key = jax.random.fold_in(key, 11)
    cell_key = jax.random.fold_in(key, 12)
    level = jax.random.randint(level_key, (1, MARKERS), 1, 1024, dtype=jnp.int32)
    cell = jax.random.randint(cell_key, (REF, MARKERS), 0, 1024, dtype=jnp.int32)
    return (cell < level).astype(jnp.int32)


def draw_posterior(key, part):
    chooser = jax.random.uniform(jax.random.fold_in(key, 21), (ANCH * N_MK, TGT, REF), jnp.float32)
    chance = 16.0 / REF
    peak = 0.25 + 0.74 * (chooser / chance)
    floor_low = jnp.log(1e-05)
    floor_high = jnp.log(0.0001)
    rest = jnp.clip((chooser - chance) / (1.0 - chance), 0.0, 1.0)
    floor = jnp.exp(floor_low + rest * (floor_high - floor_low))
    values = jnp.where(chooser < chance, peak, floor)
    return values.astype(jnp.bfloat16)


def setup_inputs(seed: int = 0) -> dict:
    key_list = jax.random.split(jax.random.key(seed), 4)
    posterior = draw_posterior(jax.random.fold_in(key_list[3], 71), 0)
    alleles = draw_alleles(jax.random.fold_in(key_list[3], 71), 0)
    owner_map = draw_owner_map(jax.random.fold_in(key_list[3], 71), 0)
    return {"posterior": posterior, "alleles": alleles, "owner_map": owner_map}


def interpolate(numerator, denominator):
    anchors = numerator.shape[0]
    intervals = anchors - 1
    block_width = numerator.shape[-1]
    marker_span = block_width // intervals
    ratios = numerator / denominator[:, :, None]
    column = jnp.arange(block_width, dtype=jnp.int32)
    interval = column // marker_span
    weight = ((column % marker_span).astype(jnp.float32) + 0.5) / marker_span
    picker = (interval[None, :] == jnp.arange(intervals, dtype=jnp.int32)[:, None]).astype(jnp.float32)
    left_part = jnp.sum(picker[:, None, :] * ratios[:-1], axis=0)
    right_part = jnp.sum(picker[:, None, :] * ratios[1:], axis=0)
    return (1.0 - weight) * left_part + weight * right_part


def positions(owner_map, devices, per_device):
    owner_table = (owner_map[:, None] == jnp.arange(devices, dtype=jnp.int32)[None, :]).astype(jnp.int32)
    owner_rank = jnp.sum(jnp.cumsum(owner_table, axis=0) * owner_table, axis=1) - 1
    return (owner_map * per_device + owner_rank).astype(jnp.int32)


def reference(posterior, alleles, owner_map):
    allele_bf = alleles.astype(jnp.bfloat16)
    unit_vector = jnp.ones((REF,), jnp.bfloat16)

    def one_anchor(index):
        group = (index // ANCH).astype(jnp.int32)
        matrix = lax.dynamic_index_in_dim(posterior, index, 0, keepdims=False)
        columns = lax.dynamic_slice_in_dim(allele_bf, group * MB, MB, 1)
        top = jnp.dot(matrix, columns, preferred_element_type=jnp.float32)
        bottom = jnp.dot(matrix, unit_vector, preferred_element_type=jnp.float32)
        return top, bottom

    numerator, denominator = lax.map(one_anchor, jnp.arange(ANCH * N_MK, dtype=jnp.int32))
    numerator = numerator.reshape(N_MK, ANCH, TGT, MB)
    denominator = denominator.reshape(N_MK, ANCH, TGT)
    block_dose = jax.vmap(interpolate)(numerator, denominator)
    all_markers = jnp.transpose(block_dose, (1, 0, 2)).reshape(TGT, MARKERS)
    row_of = positions(owner_map, N_HAP * N_MK, TOWN)
    return jnp.zeros((TGT, MARKERS), jnp.float32).at[row_of].set(all_markers)
```

```python
import functools

import jax
import jax.numpy as jnp
from jax import lax
from jax.experimental import pallas as pl
from jax.experimental.pallas import tpu as pltpu
from jax.sharding import PartitionSpec as P

LANES = 128
CORES = 2
GROUPS = 2
SIDES = 2
MESH = pl.DeviceIdType.MESH
F32 = jnp.float32
BF16 = jnp.bfloat16


def block_transpose(tiles, width):
    lane = lax.broadcasted_iota(jnp.int32, tiles[0].shape, 1) // width
    count = len(tiles)
    bit = 1
    while bit < count:
        swapped = list(tiles)
        low = lane // bit % 2 == 0
        for i in range(count):
            if i & bit == 0:
                a, b = tiles[i], tiles[i + bit]
                swapped[i] = jnp.where(low, a, pltpu.roll(b, bit * width, 1))
                swapped[i + bit] = jnp.where(low, pltpu.roll(a, LANES - bit * width, 1), b)
        tiles = swapped
        bit *= 2
    return tiles


def kernel(
    hap_count,
    mk_count,
    steps,
    post_hbm,
    allele_hbm,
    owner_hbm,
    out_ref,
    post,
    allele,
    owner,
    weights,
    choose,
    held,
    parts,
    mine,
    pair_in,
    reduced,
    inbox,
    stack,
    post_sem,
    small_sem,
    pair_send,
    pair_recv,
    chip_send,
    chip_recv,
):
    anchors, targets, refs = post.shape
    block = allele.shape[0]
    intervals = anchors - 1
    span = block // intervals
    local = intervals // GROUPS
    blocks = local * SIDES
    width = LANES // blocks
    pitch = 2 * span
    half = blocks * pitch
    rows_sent = span + 1
    chips = hap_count // CORES
    devices = hap_count * mk_count
    per_device = targets // devices
    per_chip = CORES * mk_count
    tiles_per_chip = per_chip // blocks
    chunk = targets // steps
    sent = pl.ds(0, rows_sent)

    hap, mk = lax.axis_index("hap"), lax.axis_index("mk")
    chip, core = hap // CORES, hap % CORES
    partner = {"hap": chip * CORES + 1 - core, "mk": mk}

    def place(shift):
        return (mk + shift) % mk_count

    def peer(step, shift):
        return {"hap": ((chip + step) % chips) * CORES + 1 - core, "mk": place(shift)}

    allele_copy = pltpu.make_async_copy(allele_hbm, allele, small_sem.at[0])
    owner_copy = pltpu.make_async_copy(owner_hbm, owner, small_sem.at[1])
    allele_copy.start()
    owner_copy.start()
    post_copies = {}
    for g in range(GROUPS):
        first = g * local + (g > 0)
        taken = pl.ds(first, (g + 1) * local + 1 - first)
        for i in range(steps):
            rows = pl.ds(i * chunk, chunk)
            copy = pltpu.make_async_copy(
                post_hbm.at[taken, rows, :], post.at[taken, rows, :], post_sem.at[g, i]
            )
            copy.start()
            post_copies[g, i] = copy

    barrier = pltpu.get_barrier_semaphore()
    for step in range(chips):
        for shift in range(mk_count):
            pl.semaphore_signal(barrier, inc=1, device_id=peer(step, shift), device_id_type=MESH)

    order = sorted(range(1, chips), key=lambda s: abs(s - chips // 2 - 0.5)) + [0]

    allele_copy.wait()
    lane = lax.broadcasted_iota(jnp.int32, (block, LANES), 1) % half
    marker = lax.broadcasted_iota(jnp.int32, (block, LANES), 0)
    which, within = lane // pitch, lane % pitch
    allele_bf = allele[...].astype(F32).astype(BF16)
    row_lane = lax.broadcasted_iota(jnp.int32, (1, LANES), 1) % half
    row_which, row_within = row_lane // pitch, row_lane % pitch
    slots = []
    for g in range(GROUPS):
        wanted = (g * local + which // SIDES) * span + within
        spread = ((marker == wanted) & (within < span)).astype(F32).astype(BF16)
        wide = lax.dot_general(
            allele_bf, spread, (((0,), (0,)), ((), ())), preferred_element_type=F32
        )
        for k in range(g * local, (g + 1) * local + 1):
            inside = (g * local + row_which // SIDES + row_which % SIDES == k).astype(F32)
            ones = inside * (row_within == span).astype(F32)
            weights[len(slots)] = (wide * inside + ones).astype(BF16)
            slots.append((g, k))

    owner_copy.wait()
    owners = owner[...]
    table = (lax.broadcasted_iota(jnp.int32, (devices, targets), 0) == owners).astype(F32)
    before = (
        lax.broadcasted_iota(jnp.int32, (LANES, LANES), 0)
        < lax.broadcasted_iota(jnp.int32, (LANES, LANES), 1)
    ).astype(F32).astype(BF16)
    carry = jnp.zeros((devices, 1), F32)
    ranks = []
    for b in range(targets // LANES):
        piece = table[:, b * LANES : (b + 1) * LANES]
        count = jnp.dot(piece.astype(BF16), before, preferred_element_type=F32) + carry
        ranks.append(jnp.sum(piece * count, axis=0, keepdims=True))
        carry = carry + jnp.sum(piece, axis=1, keepdims=True)
    row_of = owners.astype(F32) * width + jnp.concatenate(ranks, axis=1)

    def fill_choose(step):
        for j in range(tiles_per_chip):
            first = (((chip + step) % chips) * tiles_per_chip + j) * LANES
            wanted = (lax.broadcasted_iota(jnp.int32, (LANES, targets), 0) + first).astype(F32)
            choose[step * tiles_per_chip + j] = (wanted == row_of).astype(F32).astype(BF16)

    def split(g, rows, total):
        high = total.astype(BF16)
        low = (total - high.astype(F32)).astype(BF16)
        left = lax.broadcasted_iota(jnp.int32, total.shape, 1) < half
        parts[g, rows, :] = jnp.where(left, high.astype(F32), low.astype(F32)).astype(BF16)

    def multiply(g, i):
        rows = pl.ds(i * chunk, chunk)
        post_copies[g, i].wait()
        total = held[rows, :] if g else jnp.zeros((chunk, LANES), F32)
        for k in range(g * local + (g > 0), (g + 1) * local + 1):
            mine_at = slots.index((g, k))
            if (g + 1, k) in slots:
                both = jnp.dot(
                    post[k, rows, :],
                    jnp.concatenate([weights[mine_at], weights[slots.index((g + 1, k))]], axis=1),
                    preferred_element_type=F32,
                )
                total = total + both[:, :LANES]
                held[rows, :] = both[:, LANES:]
            else:
                total = total + jnp.dot(post[k, rows, :], weights[mine_at], preferred_element_type=F32)
        split(g, rows, total)

    pair_copies = {}
    chip_copies = {}

    def send_pair(g, step):
        copies = []
        if step:
            copies.append((mine.at[g, step, core, :, sent, :], pair_in.at[g, step, :, sent, :], 0))
        else:
            for shift in range(mk_count):
                given = core if shift else 1 - core
                copies.append(
                    (
                        mine.at[g, step, given, place(shift), sent, :],
                        pair_in.at[g, step, place(shift), sent, :],
                        shift,
                    )
                )
        started = []
        for source, target, at in copies:
            copy = pltpu.make_async_remote_copy(
                src_ref=source,
                dst_ref=target,
                send_sem=pair_send.at[g, step, at],
                recv_sem=pair_recv.at[g, step, at],
                device_id=partner,
                device_id_type=MESH,
            )
            copy.start()
            started.append(copy)
        pair_copies[g, step] = started

    def permute(g, step):
        for j in range(tiles_per_chip):
            both = jnp.dot(
                choose[step * tiles_per_chip + j], parts[g], preferred_element_type=F32
            )
            turned = jnp.transpose(both)
            sums = turned[:half] + turned[half:]
            packed = block_transpose(
                [sums[q * pitch : (q + 1) * pitch] for q in range(blocks)], width
            )
            for e in range(blocks):
                index = j * blocks + e
                mine[g, step, index // mk_count, index % mk_count] = packed[e]
        send_pair(g, step)

    def pass_on(g, step):
        for copy in pair_copies[g, step]:
            copy.wait_recv()
        for shift in range(mk_count):
            at = place(shift)
            kept = 1 - core if step or shift else core
            reduced[g, step, at] = mine[g, step, kept, at] + pair_in[g, step, at]
            if step or shift:
                copy = pltpu.make_async_remote_copy(
                    src_ref=reduced.at[g, step, at, sent, :],
                    dst_ref=inbox.at[g, step, shift, sent, :],
                    send_sem=chip_send.at[g, step, shift],
                    recv_sem=chip_recv.at[g, step, shift],
                    device_id=peer(step, shift),
                    device_id_type=MESH,
                )
                copy.start()
                chip_copies[g, step, shift] = copy

    for i in range(steps):
        for step in order[i::steps]:
            fill_choose(step)
        multiply(0, i)
    pl.semaphore_wait(barrier, chips * mk_count)
    for step in order:
        permute(0, step)
    for i in range(steps):
        multiply(1, i)
    for step in order:
        pass_on(0, step)
    lag = 3
    for at, step in enumerate(order):
        permute(1, step)
        if at >= lag:
            pass_on(1, order[at - lag])
    for step in order[-lag:]:
        pass_on(1, step)

    rank = lax.broadcasted_iota(jnp.int32, (span, LANES), 0).astype(F32)
    right = (lax.broadcasted_iota(jnp.int32, (span, LANES), 1) // width % SIDES).astype(F32)
    weight = (rank + 0.5) / span
    weight = right * weight + (1.0 - right) * (1.0 - weight)
    for g in range(GROUPS):
        for shift in range(mk_count):
            total = None
            for step in reversed(order):
                if step or shift:
                    chip_copies[g, step, shift].wait_recv()
                    arrived = inbox[g, step, shift]
                else:
                    arrived = reduced[g, step, mk]
                total = arrived if total is None else total + arrived
            ratio = weight * (total[:span] / total[span : span + 1])
            source = (mk + mk_count - shift) % mk_count
            for l in range(local):
                at = source * block + (g * local + l) * span
                moved = ratio if l == 0 else pltpu.roll(ratio, LANES - l * SIDES * width, 1)
                stack[pl.ds(pl.multiple_of(at, span), span), :] = moved

    turned = jnp.transpose(stack[...])
    out_ref[...] = turned[:per_device] + turned[width : width + per_device]

    for g in range(GROUPS):
        for step in order:
            for copy in pair_copies[g, step]:
                copy.wait_send()
            for shift in range(mk_count):
                if step or shift:
                    chip_copies[g, step, shift].wait_send()


def solution(mesh):
    hap_count, mk_count = mesh.shape["hap"], mesh.shape["mk"]
    steps = 4

    def on_device(posterior, alleles, owner_map):
        anchors, targets, refs = posterior.shape
        block = alleles.shape[1]
        intervals = anchors - 1
        span = block // intervals
        chips = hap_count // CORES
        per_device = targets // (hap_count * mk_count)
        width = LANES // (intervals // GROUPS * SIDES)
        positions = width * hap_count * mk_count
        exchange = (GROUPS, chips, mk_count, 2 * span, LANES)
        scratch = [
            pltpu.VMEM(posterior.shape, BF16),
            pltpu.VMEM((block, refs), jnp.int32),
            pltpu.VMEM((1, targets), jnp.int32),
            pltpu.VMEM((anchors + GROUPS - 1, refs, LANES), BF16),
            pltpu.VMEM((positions // LANES, LANES, targets), BF16),
            pltpu.VMEM((targets, LANES), F32),
            pltpu.VMEM((GROUPS, targets, LANES), BF16),
            pltpu.VMEM((GROUPS, chips, CORES, mk_count, 2 * span, LANES), F32),
            pltpu.VMEM(exchange, F32),
            pltpu.VMEM(exchange, F32),
            pltpu.VMEM(exchange, F32),
            pltpu.VMEM((mk_count * block, LANES), F32),
            pltpu.SemaphoreType.DMA((GROUPS, steps)),
            pltpu.SemaphoreType.DMA((2,)),
        ] + [pltpu.SemaphoreType.DMA((GROUPS, chips, mk_count))] * 4
        return pl.pallas_call(
            functools.partial(kernel, hap_count, mk_count, steps),
            out_shape=jax.ShapeDtypeStruct((per_device, mk_count * block), F32),
            in_specs=[pl.BlockSpec(memory_space=pltpu.HBM)] * 3,
            out_specs=pl.BlockSpec(memory_space=pltpu.VMEM),
            scratch_shapes=scratch,
            compiler_params=pltpu.CompilerParams(
                collective_id=0, has_side_effects=True, vmem_limit_bytes=63 * 1024 * 1024
            ),
        )(posterior, alleles.T, owner_map.reshape(1, targets))

    placed = (P("mk", None, "hap"), P("hap", "mk"), P())
    return jax.shard_map(
        on_device, mesh=mesh, in_specs=placed, out_specs=P(("hap", "mk"), None), check_vma=False
    )
```

```python
import functools

import jax
import jax.numpy as jnp
from jax import lax
from jax.experimental import pallas as pl
from jax.experimental.pallas import tpu as pltpu
from jax.sharding import PartitionSpec as P

LANES = 128
CORES = 2
GROUPS = 2
SIDES = 2
MESH = pl.DeviceIdType.MESH
F32 = jnp.float32
BF16 = jnp.bfloat16


def block_transpose(tiles, width):
    lane = lax.broadcasted_iota(jnp.int32, tiles[0].shape, 1) // width
    count = len(tiles)
    bit = 1
    while bit < count:
        swapped = list(tiles)
        low = lane // bit % 2 == 0
        for i in range(count):
            if i & bit == 0:
                a, b = tiles[i], tiles[i + bit]
                swapped[i] = jnp.where(low, a, pltpu.roll(b, bit * width, 1))
                swapped[i + bit] = jnp.where(low, pltpu.roll(a, LANES - bit * width, 1), b)
        tiles = swapped
        bit *= 2
    return tiles


def kernel(
    hap_count,
    mk_count,
    steps,
    post_hbm,
    allele_hbm,
    owner_hbm,
    out_ref,
    post,
    allele,
    owner,
    wide,
    weights,
    choose,
    held,
    parts,
    mine,
    pair_in,
    reduced,
    inbox,
    stack,
    post_sem,
    small_sem,
    pair_send,
    pair_recv,
    chip_send,
    chip_recv,
):
    anchors, targets, refs = post.shape
    block = allele.shape[0]
    intervals = anchors - 1
    span = block // intervals
    local = intervals // GROUPS
    blocks = local * SIDES
    width = LANES // blocks
    pitch = 2 * span
    half = blocks * pitch
    chips = hap_count // CORES
    devices = hap_count * mk_count
    per_device = targets // devices
    per_chip = CORES * mk_count
    tiles_per_chip = per_chip // blocks
    chunk = targets // steps
    sent = pl.ds(0, span + 1)
    far = chips * mk_count - 1

    hap, mk = lax.axis_index("hap"), lax.axis_index("mk")
    chip, core = hap // CORES, hap % CORES
    partner = {"hap": chip * CORES + 1 - core, "mk": mk}

    def place(shift):
        return (mk + shift) % mk_count

    def slot(step, shift):
        return (step - 1) % chips * mk_count + mk_count - 1 - shift

    def peer(step, shift):
        return {"hap": ((chip + step) % chips) * CORES + 1 - core, "mk": place(shift)}

    def groups_of(k):
        return [g for g in range(GROUPS) if g * local <= k <= (g + 1) * local]

    allele_copy = pltpu.make_async_copy(allele_hbm, allele, small_sem.at[0])
    owner_copy = pltpu.make_async_copy(owner_hbm, owner, small_sem.at[1])
    allele_copy.start()
    owner_copy.start()
    post_copies = {}
    for k in range(anchors):
        for i in range(steps):
            rows = pl.ds(i * chunk, chunk)
            post_copies[k, i] = pltpu.make_async_copy(
                post_hbm.at[k, rows, :], post.at[k, rows, :], post_sem.at[k, i]
            )
    for i in range(steps):
        post_copies[0, i].start()

    barrier = pltpu.get_barrier_semaphore()
    for step in range(chips):
        for shift in range(mk_count):
            pl.semaphore_signal(barrier, inc=1, device_id=peer(step, shift), device_id_type=MESH)

    order = list(range(1, chips)) + [0]

    lane = lax.broadcasted_iota(jnp.int32, (block, GROUPS * LANES), 1)
    marker = lax.broadcasted_iota(jnp.int32, (block, GROUPS * LANES), 0)
    which, within = lane % half // pitch, lane % pitch
    wanted = (lane // LANES * local + which // SIDES) * span + within
    spread = ((marker == wanted) & (within < span)).astype(F32).astype(BF16)
    with jax.named_scope("allele_wait"):
        allele_copy.wait()
        for at, copy in post_copies.items():
            if at[0]:
                copy.start()
    wide[...] = lax.dot_general(
        allele[...].astype(F32).astype(BF16),
        spread,
        (((0,), (0,)), ((), ())),
        preferred_element_type=F32,
    ).astype(BF16)

    def columns(k):
        groups = groups_of(k)
        return pl.ds(groups[0] * LANES, len(groups) * LANES)

    def fill_weights(k):
        groups = groups_of(k)
        lanes = lax.broadcasted_iota(jnp.int32, (1, len(groups) * LANES), 1) + groups[0] * LANES
        at = lanes % half // pitch
        inside = (lanes // LANES * local + at // SIDES + at % SIDES == k).astype(F32)
        ones = (inside * (lanes % pitch == span).astype(F32)).astype(BF16)
        weights[k, :, columns(k)] = wide[:, columns(k)] * inside.astype(BF16) + ones

    def fill_choose(batch, row_of):
        for step in batch:
            for j in range(tiles_per_chip):
                first = (((chip + step) % chips) * tiles_per_chip + j) * LANES
                wanted = (lax.broadcasted_iota(jnp.int32, (LANES, targets), 0) + first).astype(F32)
                choose[pl.ds((step * tiles_per_chip + j) * LANES, LANES), :] = (wanted == row_of).astype(F32).astype(BF16)

    def wait_post(k, i):
        with jax.named_scope(f"wait{k}{i}"):
            post_copies[k, i].wait()

    def multiply(k, i):
        piece = chunk // 2
        halves = [pl.ds(i * chunk + n * piece, piece) for n in range(2)]
        outs = [
            jnp.dot(post[k, rows, :], weights[k, :, columns(k)], preferred_element_type=F32)
            for rows in halves
        ]
        for rows, out in zip(halves, outs):
            for n, g in enumerate(groups_of(k)):
                total = out[:, n * LANES : (n + 1) * LANES]
                if k > g * local:
                    total = total + held[g, rows, :]
                if k < (g + 1) * local:
                    held[g, rows, :] = total
                else:
                    high = total.astype(BF16)
                    low = (total - high.astype(F32)).astype(BF16)
                    left = lax.broadcasted_iota(jnp.int32, total.shape, 1) < half
                    both = jnp.where(left, high.astype(F32), low.astype(F32))
                    parts[g, rows, :] = both.astype(BF16)

    def pair_copy(source, target, g):
        return pltpu.make_async_remote_copy(
            src_ref=source,
            dst_ref=target,
            send_sem=pair_send.at[g],
            recv_sem=pair_recv.at[g],
            device_id=partner,
            device_id_type=MESH,
        )

    def chip_copy(source, target, g, device):
        return pltpu.make_async_remote_copy(
            src_ref=source,
            dst_ref=target,
            send_sem=chip_send.at[g],
            recv_sem=chip_recv.at[g],
            device_id=device,
            device_id_type=MESH,
        )

    def send_pair(g):
        for step in order:
            if step:
                pair_copy(
                    mine.at[g, step, core, :, sent, :], pair_in.at[g, step, :, sent, :], g
                ).start()
                continue
            for shift in range(mk_count):
                given = core if shift else 1 - core
                at = place(shift)
                pair_copy(
                    mine.at[g, step, given, at, sent, :], pair_in.at[g, step, at, sent, :], g
                ).start()

    def whole_pair(g):
        return pair_copy(mine.at[g, :, core, :, sent, :], pair_in.at[g, :, :, sent, :], g)

    def whole_chip(g):
        taken = pl.ds(0, far)
        return chip_copy(
            reduced.at[g, taken, sent, :], inbox.at[g, taken, sent, :], g, peer(1, 0)
        )

    def permute(g):
        tiles = [(step, j) for step in range(chips) for j in range(tiles_per_chip)]
        batch = min(4, len(tiles))
        for first in range(0, len(tiles), batch):
            out = jnp.dot(
                choose[first * LANES : (first + batch) * LANES, :],
                parts[g],
                preferred_element_type=F32,
            )
            for n, (step, j) in enumerate(tiles[first : first + batch]):
                turned = jnp.transpose(out[n * LANES : (n + 1) * LANES])
                sums = turned[:half] + turned[half:]
                packed = block_transpose(
                    [sums[q * pitch : (q + 1) * pitch] for q in range(blocks)], width
                )
                for e in range(blocks):
                    index = j * blocks + e
                    mine[g, step, index // mk_count, index % mk_count] = packed[e]

    def pass_on(g):
        whole_pair(g).wait_recv()
        for step in order:
            for shift in reversed(range(mk_count)):
                at = place(shift)
                kept = 1 - core if step or shift else core
                to = slot(step, shift)
                reduced[g, to] = mine[g, step, kept, at] + pair_in[g, step, at]
                if step or shift:
                    chip_copy(
                        reduced.at[g, to, sent, :], inbox.at[g, to, sent, :], g, peer(step, shift)
                    ).start()

    fill_weights(0)
    with jax.named_scope("owner_wait"):
        owner_copy.wait()
    wait_post(0, 0)
    with jax.named_scope("multiply0"):
        multiply(0, 0)
        owners = owner[...]
        table = (lax.broadcasted_iota(jnp.int32, (devices, targets), 0) == owners).astype(F32)
        before = (
            lax.broadcasted_iota(jnp.int32, (LANES, LANES), 0)
            < lax.broadcasted_iota(jnp.int32, (LANES, LANES), 1)
        ).astype(F32).astype(BF16)
        carry = jnp.zeros((devices, 1), F32)
        ranks = []
        for b in range(targets // LANES):
            piece = table[:, b * LANES : (b + 1) * LANES]
            count = jnp.dot(piece.astype(BF16), before, preferred_element_type=F32) + carry
            ranks.append(jnp.sum(piece * count, axis=0, keepdims=True))
            carry = carry + jnp.sum(piece, axis=1, keepdims=True)
        row_of = owners.astype(F32) * width + jnp.concatenate(ranks, axis=1)
        fill_weights(1)
        for i in range(1, steps):
            wait_post(0, i)
            multiply(0, i)
        fill_weights(2)
    early = local * steps
    done = 0
    for k in range(1, local + 1):
        with jax.named_scope(f"multiply{k}"):
            for i in range(steps):
                wait_post(k, i)
            for i in range(steps):
                fill_choose(order[done::early], row_of)
                done += 1
                multiply(k, i)
            if k + 2 < anchors:
                fill_weights(k + 2)
    tail = [(k, i) for k in range(local + 1, anchors) for i in range(steps)]
    wait_post(*tail[0])
    with jax.named_scope("permuteA"):
        permute(0)
        multiply(*tail[0])
    with jax.named_scope("barrier"):
        pl.semaphore_wait(barrier, far + 1)
    with jax.named_scope("sendA"):
        send_pair(0)
    with jax.named_scope("multiplyB"):
        for k, i in tail[1:]:
            wait_post(k, i)
        for k, i in tail[1:]:
            multiply(k, i)
    with jax.named_scope("passA"):
        pass_on(0)
    with jax.named_scope("permuteB"):
        permute(1)
    with jax.named_scope("sendB"):
        send_pair(1)
    with jax.named_scope("passB"):
        pass_on(1)

    rank = lax.broadcasted_iota(jnp.int32, (span, LANES), 0).astype(F32)
    right = (lax.broadcasted_iota(jnp.int32, (span, LANES), 1) // width % SIDES).astype(F32)
    weight = (rank + 0.5) / span
    weight = right * weight + (1.0 - right) * (1.0 - weight)
    for g in range(GROUPS):
        with jax.named_scope(f"gather{g}"):
            whole_chip(g).wait_recv()
        for shift in range(mk_count):
            total = None
            for step in reversed(order):
                at = slot(step, shift)
                arrived = inbox[g, at] if step or shift else reduced[g, at]
                total = arrived if total is None else total + arrived
            ratio = weight * (total[:span] / total[span : span + 1])
            source = (mk + mk_count - shift) % mk_count
            for l in range(local):
                at = source * block + (g * local + l) * span
                moved = ratio if l == 0 else pltpu.roll(ratio, LANES - l * SIDES * width, 1)
                stack[pl.ds(pl.multiple_of(at, span), span), :] = moved
    with jax.named_scope("finish"):
        turned = jnp.transpose(stack[...])
        out_ref[...] = turned[:per_device] + turned[width : width + per_device]
    with jax.named_scope("drain"):
        for g in range(GROUPS):
            whole_pair(g).wait_send()
            whole_chip(g).wait_send()


def solution(mesh):
    hap_count, mk_count = mesh.shape["hap"], mesh.shape["mk"]
    steps = 2

    def on_device(posterior, alleles, owner_map):
        anchors, targets, refs = posterior.shape
        block = alleles.shape[1]
        intervals = anchors - 1
        span = block // intervals
        chips = hap_count // CORES
        per_device = targets // (hap_count * mk_count)
        width = LANES // (intervals // GROUPS * SIDES)
        positions = width * hap_count * mk_count
        slots = (GROUPS, chips * mk_count, 2 * span, LANES)
        scratch = [
            pltpu.VMEM(posterior.shape, BF16),
            pltpu.VMEM((block, refs), jnp.int32),
            pltpu.VMEM((1, targets), jnp.int32),
            pltpu.VMEM((refs, GROUPS * LANES), BF16),
            pltpu.VMEM((anchors, refs, GROUPS * LANES), BF16),
            pltpu.VMEM((positions, targets), BF16),
            pltpu.VMEM((GROUPS, targets, LANES), F32),
            pltpu.VMEM((GROUPS, targets, LANES), BF16),
            pltpu.VMEM((GROUPS, chips, CORES, mk_count, 2 * span, LANES), F32),
            pltpu.VMEM((GROUPS, chips, mk_count, 2 * span, LANES), F32),
            pltpu.VMEM(slots, F32),
            pltpu.VMEM(slots, F32),
            pltpu.VMEM((mk_count * block, LANES), F32),
            pltpu.SemaphoreType.DMA((anchors, steps)),
            pltpu.SemaphoreType.DMA((2,)),
        ] + [pltpu.SemaphoreType.DMA((GROUPS,))] * 4
        return pl.pallas_call(
            functools.partial(kernel, hap_count, mk_count, steps),
            out_shape=pltpu.VMEM((per_device, mk_count * block), F32),
            in_specs=[pl.BlockSpec(memory_space=pltpu.HBM)] * 3,
            out_specs=pl.BlockSpec(memory_space=pltpu.VMEM),
            scratch_shapes=scratch,
            compiler_params=pltpu.CompilerParams(
                collective_id=0, has_side_effects=True, vmem_limit_bytes=60000000
            ),
        )(posterior, alleles.T, owner_map.reshape(1, targets))

    placed = (P("mk", None, "hap"), P("hap", "mk"), P())
    return jax.shard_map(
        on_device, mesh=mesh, in_specs=placed, out_specs=P(("hap", "mk"), None), check_vma=False
    )
```

```python
import functools

import jax
import jax.numpy as jnp
from jax import lax
from jax.experimental import pallas as pl
from jax.experimental.pallas import tpu as pltpu
from jax.sharding import PartitionSpec as P

LANES = 128
CORES = 2
GROUPS = 2
SIDES = 2
MESH = pl.DeviceIdType.MESH
F32 = jnp.float32
BF16 = jnp.bfloat16


def block_transpose(tiles, width):
    lane = lax.broadcasted_iota(jnp.int32, tiles[0].shape, 1) // width
    count = len(tiles)
    bit = 1
    while bit < count:
        swapped = list(tiles)
        low = lane // bit % 2 == 0
        for i in range(count):
            if i & bit == 0:
                a, b = tiles[i], tiles[i + bit]
                swapped[i] = jnp.where(low, a, pltpu.roll(b, bit * width, 1))
                swapped[i + bit] = jnp.where(low, pltpu.roll(a, LANES - bit * width, 1), b)
        tiles = swapped
        bit *= 2
    return tiles


def kernel(
    hap_count,
    mk_count,
    post_hbm,
    allele_hbm,
    owner_hbm,
    out_ref,
    post,
    allele,
    owner,
    wide,
    weights,
    held,
    parts,
    mine,
    pair_in,
    reduced,
    inbox,
    stack,
    post_sem,
    small_sem,
    pair_send,
    pair_recv,
    chip_send,
    chip_recv,
):
    anchors, targets, refs = post.shape
    block = allele.shape[0]
    intervals = anchors - 1
    span = block // intervals
    local = intervals // GROUPS
    blocks = local * SIDES
    width = LANES // blocks
    values = GROUPS * span
    chips = hap_count // CORES
    devices = hap_count * mk_count
    per_device = targets // devices
    tiles_per_chip = CORES * mk_count // blocks
    sent = pl.ds(0, span + 1)
    far = chips * mk_count - 1

    hap, mk = lax.axis_index("hap"), lax.axis_index("mk")
    chip, core = hap // CORES, hap % CORES
    partner = {"hap": chip * CORES + 1 - core, "mk": mk}

    def place(shift):
        return (mk + shift) % mk_count

    def slot(step, shift):
        return (step - 1) % chips * mk_count + mk_count - 1 - shift

    def peer(step, shift):
        return {"hap": ((chip + step) % chips) * CORES + 1 - core, "mk": place(shift)}

    allele_copy = pltpu.make_async_copy(allele_hbm, allele, small_sem.at[0])
    owner_copy = pltpu.make_async_copy(owner_hbm, owner, small_sem.at[1])
    allele_copy.start()
    owner_copy.start()
    post_copies = [
        pltpu.make_async_copy(post_hbm.at[k], post.at[k], post_sem.at[k]) for k in range(anchors)
    ]
    for copy in post_copies:
        copy.start(priority=1)

    barrier = pltpu.get_barrier_semaphore()
    for step in range(chips):
        for shift in range(mk_count):
            pl.semaphore_signal(barrier, inc=1, device_id=peer(step, shift), device_id_type=MESH)

    def parts_of(lane):
        at, within = lane // width, lane % width
        is_value = within < values
        group = within // span % GROUPS
        interval = group * local + at // SIDES
        used = is_value | (within % span == 0)
        return interval, interval + at % SIDES, within % span, is_value, used

    lane = lax.broadcasted_iota(jnp.int32, (block, LANES), 1)
    marker = lax.broadcasted_iota(jnp.int32, (block, LANES), 0)
    interval, _, rank, is_value, _ = parts_of(lane)
    spread = ((marker == interval * span + rank) & is_value).astype(F32).astype(BF16)
    with jax.named_scope("allele_wait"):
        allele_copy.wait()
    wide[...] = lax.dot_general(
        allele[...].astype(F32).astype(BF16),
        spread,
        (((0,), (0,)), ((), ())),
        preferred_element_type=F32,
    ).astype(BF16)

    _, anchor, _, row_value, row_used = parts_of(lax.broadcasted_iota(jnp.int32, (1, LANES), 1))

    def fill_weights(k):
        inside = ((anchor == k) & row_used).astype(F32)
        ones = inside * (1.0 - row_value.astype(F32))
        weights[k] = wide[...] * inside.astype(BF16) + ones.astype(BF16)

    def multiply(k):
        half = targets // 2
        high_lanes, low_lanes = pl.ds(0, LANES), pl.ds(LANES, LANES)
        for n in range(2):
            rows = pl.ds(n * half, half)
            total = jnp.dot(post[k, rows, :], weights[k], preferred_element_type=F32)
            if k % (local + 1):
                total = total + held[rows, :]
            if k == anchors - 1:
                total = total + parts[rows, low_lanes].astype(F32)
                total = total + parts[rows, high_lanes].astype(F32)
            if k in (local, anchors - 1):
                high = total.astype(BF16)
                parts[rows, high_lanes] = high
                parts[rows, low_lanes] = (total - high.astype(F32)).astype(BF16)
            else:
                held[rows, :] = total

    def pair_copy(source, target, g):
        return pltpu.make_async_remote_copy(
            src_ref=source,
            dst_ref=target,
            send_sem=pair_send.at[g],
            recv_sem=pair_recv.at[g],
            device_id=partner,
            device_id_type=MESH,
        )

    def chip_copy(source, target, g, device):
        return pltpu.make_async_remote_copy(
            src_ref=source,
            dst_ref=target,
            send_sem=chip_send.at[g],
            recv_sem=chip_recv.at[g],
            device_id=device,
            device_id_type=MESH,
        )

    def send_pair(g):
        for step in every:
            if step:
                pair_copy(
                    mine.at[g, step, core, :, sent, :], pair_in.at[g, step, :, sent, :], g
                ).start()
                continue
            for shift in range(mk_count):
                given = core if shift else 1 - core
                at = place(shift)
                pair_copy(
                    mine.at[g, step, given, at, sent, :], pair_in.at[g, step, at, sent, :], g
                ).start()

    def whole_pair(g):
        return pair_copy(mine.at[g, :, core, :, sent, :], pair_in.at[g, :, :, sent, :], g)

    def whole_chip(g):
        taken = pl.ds(0, far)
        return chip_copy(
            reduced.at[g, taken, sent, :], inbox.at[g, taken, sent, :], g, peer(1, 0)
        )

    def permute(g):
        tiles = [(step, j) for step in every for j in range(tiles_per_chip)]
        batch = 4
        for at in range(0, len(tiles), batch):
            now = tiles[at : at + batch]
            chosen = []
            for step, j in now:
                first = (((chip + step) % chips) * tiles_per_chip + j) * LANES
                wanted = (lax.broadcasted_iota(jnp.int32, (LANES, targets), 0) + first).astype(F32)
                chosen.append((wanted == row_of).astype(F32).astype(BF16))
            out = jnp.dot(
                jnp.concatenate(chosen, axis=0), parts[...], preferred_element_type=F32
            )
            out = out[:, :LANES] + out[:, LANES:]
            for n, (step, j) in enumerate(now):
                turned = jnp.transpose(out[n * LANES : (n + 1) * LANES])
                tall = []
                for q in range(blocks):
                    top = q * width + g * span
                    bottom = top + values
                    tall.append(
                        jnp.concatenate([turned[top : top + span], turned[bottom : bottom + span]])
                    )
                packed = block_transpose(tall, width)
                for e in range(blocks):
                    index = j * blocks + e
                    mine[g, step, index // mk_count, index % mk_count] = packed[e]

    def pass_on(g):
        whole_pair(g).wait_recv()
        for step in every[1:] + every[:1]:
            for shift in reversed(range(mk_count)):
                at = place(shift)
                kept = 1 - core if step or shift else core
                to = slot(step, shift)
                reduced[g, to] = mine[g, step, kept, at] + pair_in[g, step, at]
                if step or shift:
                    chip_copy(
                        reduced.at[g, to, sent, :], inbox.at[g, to, sent, :], g, peer(step, shift)
                    ).start()

    fill_weights(0)
    with jax.named_scope("owner_wait"):
        owner_copy.wait()
    owners = owner[...]
    table = (lax.broadcasted_iota(jnp.int32, (devices, targets), 0) == owners).astype(F32)
    before = (
        lax.broadcasted_iota(jnp.int32, (LANES, LANES), 0)
        < lax.broadcasted_iota(jnp.int32, (LANES, LANES), 1)
    ).astype(F32).astype(BF16)
    carry = jnp.zeros((devices, 1), F32)
    ranks = []
    for b in range(targets // LANES):
        piece = table[:, b * LANES : (b + 1) * LANES]
        count = jnp.dot(piece.astype(BF16), before, preferred_element_type=F32) + carry
        ranks.append(jnp.sum(piece * count, axis=0, keepdims=True))
        carry = carry + jnp.sum(piece, axis=1, keepdims=True)
    row_of = owners.astype(F32) * width + jnp.concatenate(ranks, axis=1)

    every = list(range(chips))
    for k in range(anchors):
        with jax.named_scope(f"wait{k}"):
            post_copies[k].wait()
        with jax.named_scope(f"multiply{k}"):
            if k == local + 1:
                permute(0)
            multiply(k)
            if k + 1 < anchors:
                fill_weights(k + 1)
            if k == anchors - 1:
                permute(1)
        if k == local + 1:
            with jax.named_scope("barrier"):
                pl.semaphore_wait(barrier, far + 1)
            with jax.named_scope("sendA"):
                send_pair(0)
    with jax.named_scope("sendB"):
        send_pair(1)
    with jax.named_scope("passA"):
        pass_on(0)
    with jax.named_scope("passB"):
        pass_on(1)

    rank = lax.broadcasted_iota(jnp.int32, (span, LANES), 0).astype(F32)
    right = (lax.broadcasted_iota(jnp.int32, (span, LANES), 1) // width % SIDES).astype(F32)
    weight = (rank + 0.5) / span
    weight = right * weight + (1.0 - right) * (1.0 - weight)
    for g in range(GROUPS):
        with jax.named_scope(f"gather{g}"):
            whole_chip(g).wait_recv()
        for shift in range(mk_count):
            total = None
            for step in every:
                at = slot(step, shift)
                arrived = inbox[g, at] if step or shift else reduced[g, at]
                total = arrived if total is None else total + arrived
            ratio = weight * (total[:span] / total[span : span + 1])
            source = (mk + mk_count - shift) % mk_count
            for l in range(local):
                at = source * block + (g * local + l) * span
                moved = ratio if l == 0 else pltpu.roll(ratio, LANES - l * SIDES * width, 1)
                stack[pl.ds(pl.multiple_of(at, span), span), :] = moved
    with jax.named_scope("finish"):
        turned = jnp.transpose(stack[...])
        out_ref[...] = turned[:per_device] + turned[width : width + per_device]
    with jax.named_scope("drain"):
        for g in range(GROUPS):
            whole_pair(g).wait_send()
            whole_chip(g).wait_send()


def solution(mesh):
    hap_count, mk_count = mesh.shape["hap"], mesh.shape["mk"]

    def on_device(posterior, alleles, owner_map):
        anchors, targets, refs = posterior.shape
        block = alleles.shape[1]
        intervals = anchors - 1
        span = block // intervals
        chips = hap_count // CORES
        per_device = targets // (hap_count * mk_count)
        slots = (GROUPS, chips * mk_count, 2 * span, LANES)
        scratch = [
            pltpu.VMEM(posterior.shape, BF16),
            pltpu.VMEM((block, refs), jnp.int32),
            pltpu.VMEM((1, targets), jnp.int32),
            pltpu.VMEM((refs, LANES), BF16),
            pltpu.VMEM((anchors, refs, LANES), BF16),
            pltpu.VMEM((targets, LANES), F32),
            pltpu.VMEM((targets, 2 * LANES), BF16),
            pltpu.VMEM((GROUPS, chips, CORES, mk_count, 2 * span, LANES), F32),
            pltpu.VMEM((GROUPS, chips, mk_count, 2 * span, LANES), F32),
            pltpu.VMEM(slots, F32),
            pltpu.VMEM(slots, F32),
            pltpu.VMEM((mk_count * block, LANES), F32),
            pltpu.SemaphoreType.DMA((anchors,)),
            pltpu.SemaphoreType.DMA((2,)),
        ] + [pltpu.SemaphoreType.DMA((GROUPS,))] * 4
        return pl.pallas_call(
            functools.partial(kernel, hap_count, mk_count),
            out_shape=pltpu.VMEM((per_device, mk_count * block), F32),
            in_specs=[pl.BlockSpec(memory_space=pltpu.HBM)] * 3,
            out_specs=pl.BlockSpec(memory_space=pltpu.VMEM),
            scratch_shapes=scratch,
            compiler_params=pltpu.CompilerParams(
                collective_id=0, has_side_effects=True, vmem_limit_bytes=60000000
            ),
        )(posterior, alleles.T, owner_map.reshape(1, targets))

    placed = (P("mk", None, "hap"), P("hap", "mk"), P())
    return jax.shard_map(
        on_device, mesh=mesh, in_specs=placed, out_specs=P(("hap", "mk"), None), check_vma=False
    )
```

```python
import functools

import jax
import jax.numpy as jnp
from jax import lax
from jax.experimental import pallas as pl
from jax.experimental.pallas import tpu as pltpu
from jax.sharding import PartitionSpec as P

LANES = 128
CORES = 2
GROUPS = 2
SIDES = 2
MESH = pl.DeviceIdType.MESH
F32 = jnp.float32
BF16 = jnp.bfloat16


def block_transpose(tiles, width):
    lane = lax.broadcasted_iota(jnp.int32, tiles[0].shape, 1) // width
    count = len(tiles)
    bit = 1
    while bit < count:
        swapped = list(tiles)
        low = lane // bit % 2 == 0
        for i in range(count):
            if i & bit == 0:
                a, b = tiles[i], tiles[i + bit]
                swapped[i] = jnp.where(low, a, pltpu.roll(b, bit * width, 1))
                swapped[i + bit] = jnp.where(low, pltpu.roll(a, LANES - bit * width, 1), b)
        tiles = swapped
        bit *= 2
    return tiles


def kernel(
    hap_count,
    mk_count,
    post_hbm,
    allele_hbm,
    owner_hbm,
    out_ref,
    post,
    allele,
    owner,
    wide,
    weights,
    held,
    parts,
    mine,
    pair_in,
    reduced,
    inbox,
    stack,
    post_sem,
    small_sem,
    pair_send,
    pair_recv,
    chip_send,
    chip_recv,
):
    anchors, targets, refs = post.shape
    block = allele.shape[0]
    intervals = anchors - 1
    span = block // intervals
    local = intervals // GROUPS
    blocks = local * SIDES
    width = LANES // blocks
    values = GROUPS * span
    chips = hap_count // CORES
    devices = hap_count * mk_count
    per_device = targets // devices
    tiles_per_chip = CORES * mk_count // blocks
    sent = pl.ds(0, span + 1)
    far = chips * mk_count - 1

    hap, mk = lax.axis_index("hap"), lax.axis_index("mk")
    chip, core = hap // CORES, hap % CORES
    partner = {"hap": chip * CORES + 1 - core, "mk": mk}

    def place(shift):
        return (mk + shift) % mk_count

    def slot(step, shift):
        return (step - 1) % chips * mk_count + mk_count - 1 - shift

    def peer(step, shift):
        return {"hap": ((chip + step) % chips) * CORES + 1 - core, "mk": place(shift)}

    allele_copy = pltpu.make_async_copy(allele_hbm, allele, small_sem.at[0])
    owner_copy = pltpu.make_async_copy(owner_hbm, owner, small_sem.at[1])
    allele_copy.start()
    owner_copy.start()
    post_copies = [
        pltpu.make_async_copy(post_hbm.at[k], post.at[k], post_sem.at[k]) for k in range(anchors)
    ]
    for copy in post_copies:
        copy.start(priority=1)

    barrier = pltpu.get_barrier_semaphore()
    for step in range(chips):
        for shift in range(mk_count):
            pl.semaphore_signal(barrier, inc=1, device_id=peer(step, shift), device_id_type=MESH)

    def parts_of(lane):
        at, within = lane // width, lane % width
        is_value = within < values
        group = within // span % GROUPS
        interval = group * local + at // SIDES
        used = is_value | (within % span == 0)
        return interval, interval + at % SIDES, within % span, is_value, used

    lane = lax.broadcasted_iota(jnp.int32, (block, LANES), 1)
    marker = lax.broadcasted_iota(jnp.int32, (block, LANES), 0)
    interval, _, rank, is_value, _ = parts_of(lane)
    spread = ((marker == interval * span + rank) & is_value).astype(F32).astype(BF16)
    with jax.named_scope("allele_wait"):
        allele_copy.wait()
    wide[...] = lax.dot_general(
        allele[...].astype(F32).astype(BF16),
        spread,
        (((0,), (0,)), ((), ())),
        preferred_element_type=F32,
    ).astype(BF16)

    _, anchor, _, row_value, row_used = parts_of(lax.broadcasted_iota(jnp.int32, (1, LANES), 1))

    def fill_weights(k):
        inside = ((anchor == k) & row_used).astype(F32)
        ones = inside * (1.0 - row_value.astype(F32))
        weights[k] = wide[...] * inside.astype(BF16) + ones.astype(BF16)

    def multiply(k):
        half = targets // 2
        high_lanes, low_lanes = pl.ds(0, LANES), pl.ds(LANES, LANES)
        for n in range(2):
            rows = pl.ds(n * half, half)
            total = jnp.dot(post[k, rows, :], weights[k], preferred_element_type=F32)
            if k % (local + 1):
                total = total + held[rows, :]
            if k == anchors - 1:
                total = total + parts[rows, low_lanes].astype(F32)
                total = total + parts[rows, high_lanes].astype(F32)
            if k in (local, anchors - 1):
                high = total.astype(BF16)
                parts[rows, high_lanes] = high
                parts[rows, low_lanes] = (total - high.astype(F32)).astype(BF16)
            else:
                held[rows, :] = total

    def pair_copy(source, target, g):
        return pltpu.make_async_remote_copy(
            src_ref=source,
            dst_ref=target,
            send_sem=pair_send.at[g],
            recv_sem=pair_recv.at[g],
            device_id=partner,
            device_id_type=MESH,
        )

    def chip_copy(source, target, g, device):
        return pltpu.make_async_remote_copy(
            src_ref=source,
            dst_ref=target,
            send_sem=chip_send.at[g],
            recv_sem=chip_recv.at[g],
            device_id=device,
            device_id_type=MESH,
        )

    def send_pair(g):
        for step in every:
            if step:
                pair_copy(
                    mine.at[g, step, core, :, sent, :], pair_in.at[g, step, :, sent, :], g
                ).start()
                continue
            for shift in range(mk_count):
                given = core if shift else 1 - core
                at = place(shift)
                pair_copy(
                    mine.at[g, step, given, at, sent, :], pair_in.at[g, step, at, sent, :], g
                ).start()

    def whole_pair(g):
        return pair_copy(mine.at[g, :, core, :, sent, :], pair_in.at[g, :, :, sent, :], g)

    def whole_chip(g):
        taken = pl.ds(0, far)
        return chip_copy(
            reduced.at[g, taken, sent, :], inbox.at[g, taken, sent, :], g, peer(1, 0)
        )

    def permute(g):
        tiles = [(step, j) for step in every for j in range(tiles_per_chip)]
        batch = 2
        for at in range(0, len(tiles), batch):
            now = tiles[at : at + batch]
            chosen = []
            for step, j in now:
                first = (((chip + step) % chips) * tiles_per_chip + j) * LANES
                wanted = (lax.broadcasted_iota(jnp.int32, (LANES, targets), 0) + first).astype(F32)
                chosen.append((wanted == row_of).astype(F32).astype(BF16))
            out = jnp.dot(
                jnp.concatenate(chosen, axis=0), parts[...], preferred_element_type=F32
            )
            out = out[:, :LANES] + out[:, LANES:]
            for n, (step, j) in enumerate(now):
                turned = jnp.transpose(out[n * LANES : (n + 1) * LANES])
                tall = []
                for q in range(blocks):
                    top = q * width + g * span
                    bottom = top + values
                    tall.append(
                        jnp.concatenate([turned[top : top + span], turned[bottom : bottom + span]])
                    )
                packed = block_transpose(tall, width)
                for e in range(blocks):
                    index = j * blocks + e
                    mine[g, step, index // mk_count, index % mk_count] = packed[e]

    def pass_on(g):
        whole_pair(g).wait_recv()
        for step in every[1:] + every[:1]:
            for shift in reversed(range(mk_count)):
                at = place(shift)
                kept = 1 - core if step or shift else core
                to = slot(step, shift)
                reduced[g, to] = mine[g, step, kept, at] + pair_in[g, step, at]
                if step or shift:
                    chip_copy(
                        reduced.at[g, to, sent, :], inbox.at[g, to, sent, :], g, peer(step, shift)
                    ).start()

    fill_weights(0)
    with jax.named_scope("owner_wait"):
        owner_copy.wait()
    owners = owner[...]
    table = (lax.broadcasted_iota(jnp.int32, (devices, targets), 0) == owners).astype(F32)
    before = (
        lax.broadcasted_iota(jnp.int32, (LANES, LANES), 0)
        < lax.broadcasted_iota(jnp.int32, (LANES, LANES), 1)
    ).astype(F32).astype(BF16)
    carry = jnp.zeros((devices, 1), F32)
    ranks = []
    for b in range(targets // LANES):
        piece = table[:, b * LANES : (b + 1) * LANES]
        count = jnp.dot(piece.astype(BF16), before, preferred_element_type=F32) + carry
        ranks.append(jnp.sum(piece * count, axis=0, keepdims=True))
        carry = carry + jnp.sum(piece, axis=1, keepdims=True)
    row_of = owners.astype(F32) * width + jnp.concatenate(ranks, axis=1)

    every = list(range(chips))
    for k in range(anchors):
        with jax.named_scope(f"wait{k}"):
            post_copies[k].wait()
        with jax.named_scope(f"multiply{k}"):
            if k == local + 1:
                permute(0)
            multiply(k)
            if k + 1 < anchors:
                fill_weights(k + 1)
            if k == anchors - 1:
                permute(1)
        if k == local + 1:
            with jax.named_scope("barrier"):
                pl.semaphore_wait(barrier, far + 1)
            with jax.named_scope("sendA"):
                send_pair(0)
    with jax.named_scope("sendB"):
        send_pair(1)
    with jax.named_scope("passA"):
        pass_on(0)
    with jax.named_scope("passB"):
        pass_on(1)

    rank = lax.broadcasted_iota(jnp.int32, (span, LANES), 0).astype(F32)
    right = (lax.broadcasted_iota(jnp.int32, (span, LANES), 1) // width % SIDES).astype(F32)
    weight = (rank + 0.5) / span
    weight = right * weight + (1.0 - right) * (1.0 - weight)
    for g in range(GROUPS):
        with jax.named_scope(f"gather{g}"):
            whole_chip(g).wait_recv()
        for shift in range(mk_count):
            total = None
            for step in every:
                at = slot(step, shift)
                arrived = inbox[g, at] if step or shift else reduced[g, at]
                total = arrived if total is None else total + arrived
            ratio = weight * (total[:span] / total[span : span + 1])
            source = (mk + mk_count - shift) % mk_count
            for l in range(local):
                at = source * block + (g * local + l) * span
                moved = ratio if l == 0 else pltpu.roll(ratio, LANES - l * SIDES * width, 1)
                stack[pl.ds(pl.multiple_of(at, span), span), :] = moved
    with jax.named_scope("finish"):
        turned = jnp.transpose(stack[...])
        out_ref[...] = turned[:per_device] + turned[width : width + per_device]
    with jax.named_scope("drain"):
        for g in range(GROUPS):
            whole_pair(g).wait_send()
            whole_chip(g).wait_send()


def solution(mesh):
    hap_count, mk_count = mesh.shape["hap"], mesh.shape["mk"]

    def on_device(posterior, alleles, owner_map):
        anchors, targets, refs = posterior.shape
        block = alleles.shape[1]
        intervals = anchors - 1
        span = block // intervals
        chips = hap_count // CORES
        per_device = targets // (hap_count * mk_count)
        slots = (GROUPS, chips * mk_count, 2 * span, LANES)
        scratch = [
            pltpu.VMEM(posterior.shape, BF16),
            pltpu.VMEM((block, refs), jnp.int32),
            pltpu.VMEM((1, targets), jnp.int32),
            pltpu.VMEM((refs, LANES), BF16),
            pltpu.VMEM((anchors, refs, LANES), BF16),
            pltpu.VMEM((targets, LANES), F32),
            pltpu.VMEM((targets, 2 * LANES), BF16),
            pltpu.VMEM((GROUPS, chips, CORES, mk_count, 2 * span, LANES), F32),
            pltpu.VMEM((GROUPS, chips, mk_count, 2 * span, LANES), F32),
            pltpu.VMEM(slots, F32),
            pltpu.VMEM(slots, F32),
            pltpu.VMEM((mk_count * block, LANES), F32),
            pltpu.SemaphoreType.DMA((anchors,)),
            pltpu.SemaphoreType.DMA((2,)),
        ] + [pltpu.SemaphoreType.DMA((GROUPS,))] * 4
        return pl.pallas_call(
            functools.partial(kernel, hap_count, mk_count),
            out_shape=pltpu.VMEM((per_device, mk_count * block), F32),
            in_specs=[pl.BlockSpec(memory_space=pltpu.HBM)] * 3,
            out_specs=pl.BlockSpec(memory_space=pltpu.VMEM),
            scratch_shapes=scratch,
            compiler_params=pltpu.CompilerParams(
                collective_id=0, has_side_effects=True, vmem_limit_bytes=60000000
            ),
        )(posterior, alleles.T, owner_map.reshape(1, targets))

    placed = (P("mk", None, "hap"), P("hap", "mk"), P())
    return jax.shard_map(
        on_device, mesh=mesh, in_specs=placed, out_specs=P(("hap", "mk"), None), check_vma=False
    )
```
